32 devices in a mesh: seq: 8 (over y, x, core), head: 4 (over z).
Axes of the slice: x: 2, y: 2, z: 4, core: 2. Of those that a mesh axis runs over, the one named last changes fastest.
Arguments:
- queries: bfloat16 [4096, 4096], P('seq', 'head'), may hold values from -72 to 72
- key_heads: bfloat16 [4096, 4096], P('seq', 'head'), may hold values from -6 to 6
- value_heads: bfloat16 [4096, 4096], P('seq', 'head'), may hold values from -6 to 6
- dilation: int32 [4], replicated, may hold values from 1 to 8, as said below
- window: int32 [4], replicated, may hold values from 96 to 192, as said below
Outputs:
- attended: bfloat16 [4096, 4096], P('seq', 'head')
The draws below stay inside these ranges and needn't reach their ends.
Inputs may be any that keep to these rules, and one draw needn't show every extreme that they name: dilation holds the four numbers 1, 2, 4, 8, each once. Each window lies between 96 and 192; the group whose dilation is 8 has exactly 192.
All inputs are finite; a program needn't handle non-finite values.
Results may differ from the reference program's by a relative error of at most 0.0043.
Values may be sent and summed in bfloat16 or wider, within the bound.
No kernel may reach another device: no remote copies, remote signals or barrier semaphores. Data moves between devices by JAX's collectives and lax.ppermute only.
A program may use at most 64 MiB of HBM per device.

```python
from functools import partial
import jax
import jax.numpy as jnp
from jax import lax

HEADS = 32
HS = 128
WIN = 192
GROUPS = 4
TOKENS = 4096


def group_draw(key):
    levels = jax.random.permutation(jax.random.fold_in(key, 11), GROUPS).astype(jnp.int32)
    dilation = jnp.left_shift(jnp.ones((GROUPS,), jnp.int32), levels)
    spans = jax.random.randint(jax.random.fold_in(key, 12), (GROUPS,), WIN // 2, WIN + 1, dtype=jnp.int32)
    spans = jnp.where(dilation == 8, WIN, spans).astype(jnp.int32)
    return (dilation, spans)


def draw_dilation(key, part):
    return group_draw(key)[0]


def draw_window(key, part):
    return group_draw(key)[1]


def key_draw(key):
    return jnp.clip(jax.random.normal(jax.random.fold_in(key, 21), (TOKENS, HEADS * HS), jnp.float32), -6.0, 6.0)


def draw_key_heads(key, part):
    return key_draw(key).astype(jnp.bfloat16)


def draw_queries(key, part):
    mixed = jnp.clip(jax.random.normal(jax.random.fold_in(key, 22), (TOKENS, HEADS * HS), jnp.float32), -6.0, 6.0)
    return mixed.astype(jnp.bfloat16)


def shard_levels(stream_key, dims, cuts, low, largest):
    factor_of, own = 1.0, jax.random.fold_in(stream_key, 6)
    for dim, shards_of in cuts:
        draws = jnp.exp(jax.random.uniform(jax.random.fold_in(own, dim), (shards_of,), jnp.float32, low / len(cuts), largest / len(cuts)))
        factor_of = factor_of * jnp.repeat(draws, dims[dim] // shards_of).reshape([-1 if axis == dim else 1 for axis in range(len(dims))])
    return factor_of


def noise(key, dims, scale, reach, cuts=(), kind=jnp.bfloat16):
    gain = shard_levels(key, dims, cuts, -0.22, 0.18) if cuts else 1.0
    result = jax.random.normal(key, dims, jnp.float32) * scale * gain
    return jnp.minimum(jnp.maximum(result, -reach), reach).astype(kind)


def setup_inputs(seed: int = 0) -> dict:
    keys = jax.random.split(jax.random.key(seed), 6)
    queries = draw_queries(jax.random.fold_in(keys[5], 71), 0)
    key_heads = draw_key_heads(jax.random.fold_in(keys[5], 71), 0)
    value_heads = noise(keys[2], (TOKENS, HEADS * HS), 1.0, 6.0, ((0, 8), (1, 4)))
    dilation = draw_dilation(jax.random.fold_in(keys[5], 71), 0)
    window = draw_window(jax.random.fold_in(keys[5], 71), 0)
    return dict(queries=queries, key_heads=key_heads, value_heads=value_heads, dilation=dilation, window=window)


masked_fill = -1.0e30


def group_attend(queries, key_heads, value_heads, reach_keys, degree):
    stride = 2 ** degree
    length, width = queries.shape
    heads_here = width // HS
    padding = jnp.zeros((stride * WIN, width), key_heads.dtype)
    keys_full = jnp.concatenate([padding, key_heads], axis=0)
    values_full = jnp.concatenate([padding, value_heads], axis=0)
    block_rows = min(512, length)
    per_class = block_rows // stride
    class_length = length // stride
    q_split = queries.reshape(class_length, stride, heads_here, HS)
    k_split = keys_full.reshape(class_length + WIN, stride, heads_here, HS)
    v_split = values_full.reshape(class_length + WIN, stride, heads_here, HS)
    scale = HS ** -0.5

    def one_block(number):
        opening = (number * per_class).astype(jnp.int32)
        q_block = lax.dynamic_slice_in_dim(q_split, opening, per_class, 0).astype(jnp.float32)
        k_block = lax.dynamic_slice_in_dim(k_split, opening, per_class + WIN, 0).astype(jnp.float32)
        v_block = lax.dynamic_slice_in_dim(v_split, opening, per_class + WIN, 0).astype(jnp.float32)
        scores = jnp.einsum("urhs,vrhs->rhuv", q_block, k_block) * scale
        query_index = jnp.arange(per_class, dtype=jnp.int32)[:, None]
        key_index = jnp.arange(per_class + WIN, dtype=jnp.int32)[None, :]
        distance = query_index - key_index + WIN
        inside = (distance >= 0) & (distance < reach_keys)
        position = -stride * WIN + (opening + key_index) * stride + jnp.arange(stride, dtype=jnp.int32)[:, None]
        valid = inside[None, None, :, :] & (position >= 0)[:, None, None, :]
        masked = jnp.where(valid, scores, masked_fill)
        peak = jnp.max(masked, axis=-1, keepdims=True)
        weights = jnp.where(valid, jnp.exp(masked - peak), 0.0)
        denominator = jnp.sum(weights, axis=-1)
        rounded = weights.astype(jnp.bfloat16)
        mixed = jnp.einsum("rhuv,vrhs->urhs", rounded.astype(jnp.float32), v_block)
        mixed = mixed / jnp.transpose(denominator, (2, 0, 1))[..., None]
        return mixed.astype(jnp.bfloat16).reshape(block_rows, width)

    blocks_out = lax.map(one_block, jnp.arange(length // block_rows, dtype=jnp.int32))
    return blocks_out.reshape(length, width)


def reference(queries, key_heads, value_heads, dilation, window):
    width = queries.shape[1]
    portion = width // GROUPS
    results = []
    for member in range(GROUPS):
        lower = member * portion
        upper = lower + portion
        level_index = ((dilation[member] > 1).astype(jnp.int32) + (dilation[member] > 2).astype(jnp.int32) + (dilation[member] > 4).astype(jnp.int32))
        branches = [partial(group_attend, degree=degree) for degree in range(4)]
        results.append(lax.switch(level_index, branches, queries[:, lower:upper], key_heads[:, lower:upper], value_heads[:, lower:upper], window[member]))
    return jnp.concatenate(results, axis=1)
```

```python
from functools import partial

import jax
import jax.numpy as jnp
from jax import lax
from jax.experimental import pallas as pl
from jax.experimental.pallas import tpu as pltpu
from jax.sharding import PartitionSpec as P

HS = 128
WIN = 192
LEVELS = 4
REACH = 3
LOG2E = 1.4426950408889634
masked_fill = -1e30


def tiling(level, length):
    stride = 2**level
    rows = min(128, length // stride)
    keys = -(-(rows + WIN) // 128) * 128
    return (stride, rows, keys)


def unit_list(level, length):
    stride, rows, keys = tiling(level, length)
    blocks = length // stride // rows
    lead = keys - rows
    units = []
    for residue in range(stride):
        for block in range(blocks):
            first = residue + block * rows * stride
            units.append((block, first, REACH * length + first - lead * stride))
    return units


def spread(scratch, refs, odd, relayed, partner_relayed, level, length):
    near, step_two, swapped, relay, relay_swapped, own = refs

    def put(at, ref):
        scratch[pl.ds(pl.multiple_of(at, 8), length), :] = ref[...].astype(jnp.float32)

    put(REACH * length, own)

    @pl.when(jnp.logical_or(odd == 1, level == 3))
    def _():
        put(jnp.where(odd == 1, 2 * length, 0), near)

    @pl.when(jnp.logical_and(jnp.logical_or(odd == 0, level == 3), partner_relayed == 0))
    def _():
        put(jnp.where(odd == 1, 0, 2 * length), swapped)

    @pl.when(partner_relayed == 1)
    def _():
        put(2 * length, relay_swapped)

    @pl.when(jnp.logical_and(level >= 2, relayed == 0))
    def _():
        put(length, step_two)

    @pl.when(jnp.logical_and(level >= 2, relayed == 1))
    def _():
        put(length, relay)


def score_kernel(length, scal, q_ref, *rest):
    key_refs = rest[:6]
    p_ref, t_ref, q_all, k_all, bias = rest[6:]
    level, reach_keys, seat, odd, relayed, partner_relayed = [scal[i] for i in range(6)]
    q_all[...] = q_ref[...].astype(jnp.float32)
    spread(k_all, key_refs, odd, relayed, partner_relayed, level, length)
    factor = HS ** (-0.5) * LOG2E
    for static_level in range(LEVELS):

        @pl.when(level == static_level)
        def _(static_level=static_level):
            stride, rows, keys = tiling(static_level, length)
            lead = keys - rows

            @pl.when(pl.program_id(0) == 0)
            def _():
                row = lax.broadcasted_iota(jnp.int32, (rows, keys), 0)
                col = lax.broadcasted_iota(jnp.int32, (rows, keys), 1)
                distance = row - col + lead
                inside = (distance >= 0) & (distance < reach_keys)
                for block in range(length // stride // rows):
                    there = col + (block * rows - lead) + seat * (length // stride) >= 0
                    bias[block, :rows, :keys] = jnp.where(inside & there, 0.0, masked_fill)

            for number, (block, q_first, k_first) in enumerate(unit_list(static_level, length)):
                q = q_all[pl.ds(q_first, rows, stride=stride), :].astype(jnp.bfloat16)
                k = k_all[pl.ds(k_first, keys, stride=stride), :].astype(jnp.bfloat16)
                s = lax.dot_general(
                    q, k, (((1,), (1,)), ((), ())), preferred_element_type=jnp.float32
                )
                s = s + bias[block, :rows, :keys]
                peak = jnp.max(s, axis=-1, keepdims=True)
                w = jnp.exp2((s - peak) * factor)
                total = jnp.sum(w, axis=-1, keepdims=True)
                lower = number * rows
                p_ref[0, lower : lower + rows, :keys] = w.astype(jnp.bfloat16)
                t_ref[0, lower : lower + rows, :] = jnp.broadcast_to(total, (rows, HS))


def mix_kernel(length, scal, p_ref, t_ref, *rest):
    value_refs = rest[:6]
    o_ref, v_all, o_all = rest[6:]
    level, reach_keys, seat, odd, relayed, partner_relayed = [scal[i] for i in range(6)]
    spread(v_all, value_refs, odd, relayed, partner_relayed, level, length)
    for static_level in range(LEVELS):

        @pl.when(level == static_level)
        def _(static_level=static_level):
            stride, rows, keys = tiling(static_level, length)
            for number, (block, q_first, k_first) in enumerate(unit_list(static_level, length)):
                v = v_all[pl.ds(k_first, keys, stride=stride), :].astype(jnp.bfloat16)
                lower = number * rows
                p = p_ref[0, lower : lower + rows, :keys]
                mixed = jnp.dot(p, v, preferred_element_type=jnp.float32)
                mixed = mixed / t_ref[0, lower : lower + rows, :]
                o_all[pl.ds(q_first, rows, stride=stride), :] = mixed

    o_ref[...] = o_all[...].astype(jnp.bfloat16)


def routes(count):
    relay_from = [s for s in range(3, count, 4) if s + REACH < count]
    near = [(s, s + (1 if s % 2 == 0 else REACH)) for s in range(count)]
    near = [(a, b) for a, b in near if b < count]
    two = [(s, s + 2) for s in range(count - 2) if s not in relay_from]
    relay = [(s + 3, s + 2) for s in relay_from]
    swap = [(s, s ^ 1) for s in range(2, count) if s - 2 not in relay_from]
    relay_swap = [(s + 2, s + 1) for s in relay_from]
    return near, two, relay, swap, relay_swap


def body(queries, key_heads, value_heads, dilation, window):
    length, width = queries.shape
    heads_here = width // HS
    count = lax.axis_size("seq")
    seat = lax.axis_index("seq")
    group = lax.axis_index("head")
    step = dilation[group]
    level = (step > 1).astype(jnp.int32) + (step > 2).astype(jnp.int32) + (step > 4).astype(jnp.int32)
    near, two, relay, swap, relay_swap = routes(count)
    relayed = sum([(seat == b).astype(jnp.int32) for _, b in relay], jnp.int32(0))
    partner_relayed = sum([(seat == b).astype(jnp.int32) for _, b in relay_swap], jnp.int32(0))
    scal = jnp.stack([level, window[group], seat, seat % 2, relayed, partner_relayed]).astype(jnp.int32)

    def send(value, pairs):
        return lax.ppermute(value, "seq", pairs)

    def gather(value):
        by_two = send(value, two)
        nearby = send(value, near)
        relays = send(nearby, relay)
        return nearby, by_two, send(by_two, swap), relays, send(relays, relay_swap), value

    keys = gather(key_heads)
    values = gather(value_heads)

    column = pl.BlockSpec((length, HS), lambda h, scal: (0, h))
    keys_most = max(tiling(level, length)[2] for level in range(LEVELS))
    p_spec = pl.BlockSpec((1, length, keys_most), lambda h, scal: (h, 0, 0))
    t_spec = pl.BlockSpec((1, length, HS), lambda h, scal: (h, 0, 0))
    rows_all = (REACH + 1) * length
    blocks_most = max(length // tiling(l, length)[0] // tiling(l, length)[1] for l in range(LEVELS))
    rows_most = max(tiling(l, length)[1] for l in range(LEVELS))
    params = pltpu.CompilerParams(dimension_semantics=("arbitrary",))
    weights, totals = pl.pallas_call(
        partial(score_kernel, length),
        grid_spec=pltpu.PrefetchScalarGridSpec(
            num_scalar_prefetch=1,
            grid=(heads_here,),
            in_specs=[column] * 7,
            out_specs=[p_spec, t_spec],
            scratch_shapes=[
                pltpu.VMEM((length, HS), jnp.float32),
                pltpu.VMEM((rows_all, HS), jnp.float32),
                pltpu.VMEM((blocks_most, rows_most, keys_most), jnp.float32),
            ],
        ),
        out_shape=[
            jax.ShapeDtypeStruct((heads_here, length, keys_most), jnp.bfloat16),
            jax.ShapeDtypeStruct((heads_here, length, HS), jnp.float32),
        ],
        compiler_params=params,
        name="scores",
    )(scal, queries, *keys)
    return pl.pallas_call(
        partial(mix_kernel, length),
        grid_spec=pltpu.PrefetchScalarGridSpec(
            num_scalar_prefetch=1,
            grid=(heads_here,),
            in_specs=[p_spec, t_spec] + [column] * 6,
            out_specs=column,
            scratch_shapes=[
                pltpu.VMEM((rows_all, HS), jnp.float32),
                pltpu.VMEM((length, HS), jnp.float32),
            ],
        ),
        out_shape=jax.ShapeDtypeStruct((length, width), jnp.bfloat16),
        compiler_params=params,
        name="mix",
    )(scal, weights, totals, *values)


def solution(mesh):
    return jax.shard_map(
        body,
        mesh=mesh,
        in_specs=(P("seq", "head"), P("seq", "head"), P("seq", "head"), P(), P()),
        out_specs=P("seq", "head"),
        check_vma=False,
    )
```

```python
from functools import partial

import jax
import jax.numpy as jnp
from jax import lax
from jax.experimental import pallas as pl
from jax.experimental.pallas import tpu as pltpu
from jax.sharding import PartitionSpec as P


HS = 128
WIN = 192
LEVELS = 4
REACH = 3
LOG2E = 1.4426950408889634
masked_fill = -1e30
VMEM_SCORES = 40 << 20
VMEM_MIX = 40 << 20


def tiling(level, length):
    stride = 2**level
    rows = min(128, length // stride)
    keys = -(-(rows + WIN) // 128) * 128
    return (stride, rows, keys)


def unit_list(level, length):
    stride, rows, keys = tiling(level, length)
    blocks = length // stride // rows
    lead = keys - rows
    units = []
    for residue in range(stride):
        for block in range(blocks):
            first = residue + block * rows * stride
            units.append((block, first, REACH * length + first - lead * stride))
    return units


def placing(dilation, window, count):
    seat = lax.axis_index("seq")
    group = lax.axis_index("head")
    step = dilation[group]
    level = sum((step > 2**i).astype(jnp.int32) for i in range(LEVELS - 1))
    _, _, relay, _, relay_swap = routes(count)
    relayed = sum([(seat == b).astype(jnp.int32) for _, b in relay], jnp.int32(0))
    partner_relayed = sum([(seat == b).astype(jnp.int32) for _, b in relay_swap], jnp.int32(0))
    return level, window[group], seat, lax.rem(seat, 2), relayed, partner_relayed


def spread(scratch, refs, odd, relayed, partner_relayed, level, length):
    near, step_two, swapped, relay, relay_swapped, own = refs
    columns = pl.ds(pl.multiple_of(pl.program_id(0) * HS, HS), HS)

    def put(at, ref):
        scratch[pl.ds(pl.multiple_of(at, 8), length), :] = ref[:, columns].astype(jnp.float32)

    put(REACH * length, own)

    @pl.when(jnp.logical_or(odd == 1, level == 3))
    def _():
        put(jnp.where(odd == 1, 2 * length, 0), near)

    @pl.when(jnp.logical_and(jnp.logical_or(odd == 0, level == 3), partner_relayed == 0))
    def _():
        put(jnp.where(odd == 1, 0, 2 * length), swapped)

    @pl.when(partner_relayed == 1)
    def _():
        put(2 * length, relay_swapped)

    @pl.when(jnp.logical_and(level >= 2, relayed == 0))
    def _():
        put(length, step_two)

    @pl.when(jnp.logical_and(level >= 2, relayed == 1))
    def _():
        put(length, relay)


def score_kernel(length, count, dilation, window, q_ref, *rest):
    key_refs = rest[:6]
    p_ref, t_ref, q_all, k_all, bias = rest[6:]
    level, reach_keys, seat, odd, relayed, partner_relayed = placing(dilation, window, count)
    head = pl.program_id(0)
    q_all[...] = q_ref[:, pl.ds(pl.multiple_of(head * HS, HS), HS)].astype(jnp.float32)
    spread(k_all, key_refs, odd, relayed, partner_relayed, level, length)
    factor = HS ** (-0.5) * LOG2E
    for static_level in range(LEVELS):

        @pl.when(level == static_level)
        def _(static_level=static_level):
            stride, rows, keys = tiling(static_level, length)
            lead = keys - rows

            @pl.when(pl.program_id(0) == 0)
            def _():
                row = lax.broadcasted_iota(jnp.int32, (rows, keys), 0)
                col = lax.broadcasted_iota(jnp.int32, (rows, keys), 1)
                distance = row - col + lead
                inside = (distance >= 0) & (distance < reach_keys)
                for block in range(length // stride // rows):
                    there = col + (block * rows - lead) + seat * (length // stride) >= 0
                    bias[block, :rows, :keys] = jnp.where(inside & there, 0.0, masked_fill)

            for number, (block, q_first, k_first) in enumerate(unit_list(static_level, length)):
                q = q_all[pl.ds(q_first, rows, stride=stride), :].astype(jnp.bfloat16)
                k = k_all[pl.ds(k_first, keys, stride=stride), :].astype(jnp.bfloat16)
                s = lax.dot_general(
                    q, k, (((1,), (1,)), ((), ())), preferred_element_type=jnp.float32
                )
                s = s + bias[block, :rows, :keys]
                peak = jnp.max(s, axis=-1, keepdims=True)
                w = jnp.exp2((s - peak) * factor)
                total = jnp.sum(w, axis=-1, keepdims=True)
                lower = number * rows
                p_ref[head, lower : lower + rows, :keys] = w.astype(jnp.bfloat16)
                t_ref[head, lower : lower + rows, :] = jnp.broadcast_to(total, (rows, HS))


def mix_kernel(length, count, dilation, window, p_ref, t_ref, *rest):
    value_refs = rest[:6]
    o_ref, v_all, o_all = rest[6:]
    level, _, _, odd, relayed, partner_relayed = placing(dilation, window, count)
    head = pl.program_id(0)
    spread(v_all, value_refs, odd, relayed, partner_relayed, level, length)
    for static_level in range(LEVELS):

        @pl.when(level == static_level)
        def _(static_level=static_level):
            stride, rows, keys = tiling(static_level, length)
            for number, (block, q_first, k_first) in enumerate(unit_list(static_level, length)):
                v = v_all[pl.ds(k_first, keys, stride=stride), :].astype(jnp.bfloat16)
                lower = number * rows
                p = p_ref[head, lower : lower + rows, :keys]
                mixed = jnp.dot(p, v, preferred_element_type=jnp.float32)
                mixed = mixed / t_ref[head, lower : lower + rows, :]
                o_all[pl.ds(q_first, rows, stride=stride), :] = mixed

    o_ref[...] = o_all[...].astype(jnp.bfloat16)


def routes(count):
    relay_from = [s for s in range(3, count, 4) if s + REACH < count]
    near = [(s, s + (1 if s % 2 == 0 else REACH)) for s in range(count)]
    near = [(a, b) for a, b in near if b < count]
    two = [(s, s + 2) for s in range(count - 2) if s not in relay_from]
    relay = [(s + 3, s + 2) for s in relay_from]
    swap = [(s, s ^ 1) for s in range(2, count) if s - 2 not in relay_from]
    relay_swap = [(s + 2, s + 1) for s in relay_from]
    return near, two, relay, swap, relay_swap


def body(queries, key_heads, value_heads, dilation, window):
    length, width = queries.shape
    heads_here = width // HS
    count = lax.axis_size("seq")
    near, two, relay, swap, relay_swap = routes(count)

    def send(value, pairs):
        return lax.ppermute(value, "seq", pairs)

    def gather(value):
        by_two = send(value, two)
        nearby = send(value, near)
        relays = send(nearby, relay)
        swapped = send(by_two, swap)
        relay_swapped = send(relays, relay_swap)
        return nearby, by_two, swapped, relays, relay_swapped, value

    whole = pl.BlockSpec(memory_space=pltpu.VMEM)
    keys_most = max(tiling(level, length)[2] for level in range(LEVELS))
    rows_all = (REACH + 1) * length
    blocks_most = max(length // tiling(l, length)[0] // tiling(l, length)[1] for l in range(LEVELS))
    rows_most = max(tiling(l, length)[1] for l in range(LEVELS))

    def call(kernel, operands, out_specs, out_shape, scratch_shapes, limit):
        return pl.pallas_call(
            partial(kernel, length, count),
            grid_spec=pltpu.PrefetchScalarGridSpec(
                num_scalar_prefetch=2,
                grid=(heads_here,),
                in_specs=[whole] * len(operands),
                out_specs=out_specs,
                scratch_shapes=scratch_shapes,
            ),
            out_shape=out_shape,
            compiler_params=pltpu.CompilerParams(
                dimension_semantics=("arbitrary",), vmem_limit_bytes=limit
            ),
        )(dilation, window, *operands)

    keys = gather(key_heads)
    values = gather(value_heads)
    weights, totals = call(
        score_kernel,
        (queries, *keys),
        [whole, whole],
        [
            pltpu.VMEM((heads_here, length, keys_most), jnp.bfloat16),
            pltpu.VMEM((heads_here, length, HS), jnp.float32),
        ],
        [
            pltpu.VMEM((length, HS), jnp.float32),
            pltpu.VMEM((rows_all, HS), jnp.float32),
            pltpu.VMEM((blocks_most, rows_most, keys_most), jnp.float32),
        ],
        VMEM_SCORES,
    )
    return call(
        mix_kernel,
        (weights, totals, *values),
        pl.BlockSpec((length, HS), lambda h, *_: (0, h)),
        jax.ShapeDtypeStruct((length, width), jnp.bfloat16),
        [
            pltpu.VMEM((rows_all, HS), jnp.float32),
            pltpu.VMEM((length, HS), jnp.float32),
        ],
        VMEM_MIX,
    )


def solution(mesh):

    return jax.shard_map(
        body,
        mesh=mesh,
        in_specs=(P("seq", "head"), P("seq", "head"), P("seq", "head"), P(), P()),
        out_specs=P("seq", "head"),
        check_vma=False,
    )
```

```python
from functools import partial

import jax
import jax.numpy as jnp
from jax import lax
from jax.experimental import pallas as pl
from jax.experimental.pallas import tpu as pltpu
from jax.sharding import PartitionSpec as P


HS = 128
WIN = 192
LEVELS = 4
REACH = 3
LOG2E = 1.4426950408889634
masked_fill = -1e30
VMEM_SCORES = 40 << 20
VMEM_MIX = 40 << 20


def tiling(level, length):
    stride = 2**level
    rows = min(128, length // stride)
    keys = -(-(rows + WIN) // 128) * 128
    return (stride, rows, keys)


def unit_list(level, length):
    stride, rows, keys = tiling(level, length)
    blocks = length // stride // rows
    lead = keys - rows
    units = []
    for residue in range(stride):
        for block in range(blocks):
            first = residue + block * rows * stride
            units.append((block, first, REACH * length + first - lead * stride))
    return units


def placing(dilation, window, count):
    seat = lax.axis_index("seq")
    group = lax.axis_index("head")
    step = dilation[group]
    level = sum((step > 2**i).astype(jnp.int32) for i in range(LEVELS - 1))
    _, far, _, relay, _, relay_swap = routes(count)

    def among(targets):
        return sum([(seat == b).astype(jnp.int32) for b in targets], jnp.int32(0))

    relayed = among([b for _, b in relay])
    partner_relayed = among([b for _, b in relay_swap])
    from_far = among([b for _, b in far])
    return level, window[group], seat, lax.rem(seat, 2), relayed, partner_relayed, from_far


def spread(scratch, refs, odd, relayed, partner_relayed, from_far, level, length):
    near, far, step_two, swapped, relay, relay_swapped, own = refs
    columns = pl.ds(pl.multiple_of(pl.program_id(0) * HS, HS), HS)

    def put(at, ref):
        scratch[pl.ds(pl.multiple_of(at, 8), length), :] = ref[:, columns].astype(jnp.float32)

    put(REACH * length, own)

    @pl.when(jnp.logical_and(jnp.logical_or(odd == 1, level == 3), from_far == 0))
    def _():
        put(jnp.where(odd == 1, 2 * length, 0), near)

    @pl.when(jnp.logical_and(level == 3, from_far == 1))
    def _():
        put(0, far)

    @pl.when(jnp.logical_and(jnp.logical_or(odd == 0, level == 3), partner_relayed == 0))
    def _():
        put(jnp.where(odd == 1, 0, 2 * length), swapped)

    @pl.when(partner_relayed == 1)
    def _():
        put(2 * length, relay_swapped)

    @pl.when(jnp.logical_and(level >= 2, relayed == 0))
    def _():
        put(length, step_two)

    @pl.when(jnp.logical_and(level >= 2, relayed == 1))
    def _():
        put(length, relay)


def score_kernel(length, count, dilation, window, q_ref, *rest):
    key_refs = rest[:7]
    p_ref, t_ref, q_all, k_all, bias = rest[7:]
    level, reach_keys, seat, odd, relayed, partner_relayed, from_far = placing(dilation, window, count)
    head = pl.program_id(0)
    q_all[...] = q_ref[:, pl.ds(pl.multiple_of(head * HS, HS), HS)].astype(jnp.float32)
    spread(k_all, key_refs, odd, relayed, partner_relayed, from_far, level, length)
    factor = HS ** (-0.5) * LOG2E
    for static_level in range(LEVELS):

        @pl.when(level == static_level)
        def _(static_level=static_level):
            stride, rows, keys = tiling(static_level, length)
            lead = keys - rows

            @pl.when(pl.program_id(0) == 0)
            def _():
                row = lax.broadcasted_iota(jnp.int32, (rows, keys), 0)
                col = lax.broadcasted_iota(jnp.int32, (rows, keys), 1)
                distance = row - col + lead
                inside = (distance >= 0) & (distance < reach_keys)
                for block in range(length // stride // rows):
                    there = col + (block * rows - lead) + seat * (length // stride) >= 0
                    bias[block, :rows, :keys] = jnp.where(inside & there, 0.0, masked_fill)

            for number, (block, q_first, k_first) in enumerate(unit_list(static_level, length)):
                q = q_all[pl.ds(q_first, rows, stride=stride), :].astype(jnp.bfloat16)
                k = k_all[pl.ds(k_first, keys, stride=stride), :].astype(jnp.bfloat16)
                s = lax.dot_general(
                    q, k, (((1,), (1,)), ((), ())), preferred_element_type=jnp.float32
                )
                s = s + bias[block, :rows, :keys]
                peak = jnp.max(s, axis=-1, keepdims=True)
                w = jnp.exp2((s - peak) * factor)
                total = jnp.sum(w, axis=-1, keepdims=True)
                lower = number * rows
                p_ref[head, lower : lower + rows, :keys] = w.astype(jnp.bfloat16)
                t_ref[head, lower : lower + rows, :] = jnp.broadcast_to(total, (rows, HS))


def mix_kernel(length, count, dilation, window, p_ref, t_ref, *rest):
    value_refs = rest[:7]
    o_ref, v_all, o_all = rest[7:]
    level, _, _, odd, relayed, partner_relayed, from_far = placing(dilation, window, count)
    head = pl.program_id(0)
    spread(v_all, value_refs, odd, relayed, partner_relayed, from_far, level, length)
    for static_level in range(LEVELS):

        @pl.when(level == static_level)
        def _(static_level=static_level):
            stride, rows, keys = tiling(static_level, length)
            for number, (block, q_first, k_first) in enumerate(unit_list(static_level, length)):
                v = v_all[pl.ds(k_first, keys, stride=stride), :].astype(jnp.bfloat16)
                lower = number * rows
                p = p_ref[head, lower : lower + rows, :keys]
                mixed = jnp.dot(p, v, preferred_element_type=jnp.float32)
                mixed = mixed / t_ref[head, lower : lower + rows, :]
                o_all[pl.ds(q_first, rows, stride=stride), :] = mixed

    o_ref[...] = o_all[...].astype(jnp.bfloat16)


def routes(count):
    relay_from = [s for s in range(3, count, 4) if s + REACH < count]
    near = [(s, s + 1) for s in range(0, count - 1, 2)] + [(s, s + REACH) for s in relay_from]
    far = [(s, s + REACH) for s in range(1, count - REACH, 2) if s not in relay_from]
    two = [(s, s + 2) for s in range(count - 2) if s not in relay_from]
    relay = [(s + 3, s + 2) for s in relay_from]
    swap = [(s, s ^ 1) for s in range(2, count) if s - 2 not in relay_from]
    relay_swap = [(s + 2, s + 1) for s in relay_from]
    return near, far, two, relay, swap, relay_swap


def body(queries, key_heads, value_heads, dilation, window):
    length, width = queries.shape
    heads_here = width // HS
    count = lax.axis_size("seq")
    near, far, two, relay, swap, relay_swap = routes(count)

    def send(value, pairs):
        return lax.ppermute(value, "seq", pairs)

    def gather(value):
        by_two = send(value, two)
        nearby = send(value, near)
        beyond = send(value, far)
        relays = send(nearby, relay)
        swapped = send(by_two, swap)
        relay_swapped = send(relays, relay_swap)
        return nearby, beyond, by_two, swapped, relays, relay_swapped, value

    whole = pl.BlockSpec(memory_space=pltpu.VMEM)
    keys_most = max(tiling(level, length)[2] for level in range(LEVELS))
    rows_all = (REACH + 1) * length
    blocks_most = max(length // tiling(l, length)[0] // tiling(l, length)[1] for l in range(LEVELS))
    rows_most = max(tiling(l, length)[1] for l in range(LEVELS))

    def call(kernel, operands, out_specs, out_shape, scratch_shapes, limit):
        return pl.pallas_call(
            partial(kernel, length, count),
            grid_spec=pltpu.PrefetchScalarGridSpec(
                num_scalar_prefetch=2,
                grid=(heads_here,),
                in_specs=[whole] * len(operands),
                out_specs=out_specs,
                scratch_shapes=scratch_shapes,
            ),
            out_shape=out_shape,
            compiler_params=pltpu.CompilerParams(
                dimension_semantics=("arbitrary",), vmem_limit_bytes=limit
            ),
        )(dilation, window, *operands)

    keys = gather(key_heads)
    values = gather(value_heads)
    weights, totals = call(
        score_kernel,
        (queries, *keys),
        [whole, whole],
        [
            pltpu.VMEM((heads_here, length, keys_most), jnp.bfloat16),
            pltpu.VMEM((heads_here, length, HS), jnp.float32),
        ],
        [
            pltpu.VMEM((length, HS), jnp.float32),
            pltpu.VMEM((rows_all, HS), jnp.float32),
            pltpu.VMEM((blocks_most, rows_most, keys_most), jnp.float32),
        ],
        VMEM_SCORES,
    )
    return call(
        mix_kernel,
        (weights, totals, *values),
        pl.BlockSpec((length, HS), lambda h, *_: (0, h)),
        jax.ShapeDtypeStruct((length, width), jnp.bfloat16),
        [
            pltpu.VMEM((rows_all, HS), jnp.float32),
            pltpu.VMEM((length, HS), jnp.float32),
        ],
        VMEM_MIX,
    )


def solution(mesh):
    return jax.shard_map(
        body,
        mesh=mesh,
        in_specs=(P("seq", "head"), P("seq", "head"), P("seq", "head"), P(), P()),
        out_specs=P("seq", "head"),
        check_vma=False,
    )
```

```python
from functools import partial

import jax
import jax.numpy as jnp
from jax import lax
from jax.experimental import pallas as pl
from jax.experimental.pallas import tpu as pltpu
from jax.sharding import PartitionSpec as P


HS = 128
WIN = 192
LEVELS = 4
REACH = 3
LOG2E = 1.4426950408889634
masked_fill = -1e30
VMEM_LIMIT = 40 << 20


def tiling(level, length):
    stride = 2**level
    rows = min(128, length // stride)
    keys = -(-(rows + WIN) // 128) * 128
    return (stride, rows, keys)


def unit_list(level, length):
    stride, rows, keys = tiling(level, length)
    blocks = length // stride // rows
    lead = keys - rows
    units = []
    for residue in range(stride):
        for block in range(blocks):
            first = residue + block * rows * stride
            units.append((block, first, REACH * length + first - lead * stride))
    return units


def placing(dilation, window, count):
    seat = lax.axis_index("seq")
    group = lax.axis_index("head")
    step = dilation[group]
    level = sum((step > 2**i).astype(jnp.int32) for i in range(LEVELS - 1))
    _, far, _, relay, _, relay_swap = routes(count)

    def among(targets):
        return sum([(seat == b).astype(jnp.int32) for b in targets], jnp.int32(0))

    relayed = among([b for _, b in relay])
    partner_relayed = among([b for _, b in relay_swap])
    from_far = among([b for _, b in far])
    return level, window[group], seat, lax.rem(seat, 2), relayed, partner_relayed, from_far


def spread(scratch, refs, place, length, head):
    level, _, _, odd, relayed, partner_relayed, from_far = place
    near, far, relay, relay_swapped, own, two, swap = refs

    def put(at, ref, column):
        columns = pl.ds(pl.multiple_of(column * HS, HS), HS)
        scratch[pl.ds(pl.multiple_of(at, 8), length), :] = ref[:, columns].astype(jnp.float32)

    def put_part(at, parts, wanted):
        if len(parts) == 1:
            low, ref = parts[0]

            @pl.when(wanted)
            def _():
                put(at, ref, head - low)

        else:
            (low, first), (high, second) = parts

            @pl.when(jnp.logical_and(wanted, head < high))
            def _():
                put(at, first, head - low)

            @pl.when(jnp.logical_and(wanted, head >= high))
            def _():
                put(at, second, head - high)

    put(REACH * length, own, 0)

    @pl.when(jnp.logical_and(jnp.logical_or(odd == 1, level == 3), from_far == 0))
    def _():
        put(jnp.where(odd == 1, 2 * length, 0), near, head)

    @pl.when(jnp.logical_and(level == 3, from_far == 1))
    def _():
        put(0, far, head)

    put_part(
        jnp.where(odd == 1, 0, 2 * length),
        swap,
        jnp.logical_and(jnp.logical_or(odd == 0, level == 3), partner_relayed == 0),
    )

    @pl.when(partner_relayed == 1)
    def _():
        put(2 * length, relay_swapped, head)

    put_part(length, two, jnp.logical_and(level >= 2, relayed == 0))

    @pl.when(jnp.logical_and(level >= 2, relayed == 1))
    def _():
        put(length, relay, head)


def take_refs(refs, parts):
    count = len(parts)
    two = list(zip(parts, refs[5 : 5 + count]))
    swap = list(zip(parts, refs[5 + count : 5 + 2 * count]))
    return (*refs[:5], two, swap), refs[5 + 2 * count :]


def score_kernel(length, count, first_head, parts, dilation, window, q_ref, *rest):
    key_refs, (p_ref, t_ref, q_all, k_all, bias) = take_refs(rest, parts)
    place = placing(dilation, window, count)
    level, reach_keys, seat = place[:3]
    head = pl.program_id(0) + first_head
    q_all[...] = q_ref[...].astype(jnp.float32)
    spread(k_all, key_refs, place, length, head)
    factor = HS ** (-0.5) * LOG2E
    for static_level in range(LEVELS):

        @pl.when(level == static_level)
        def _(static_level=static_level):
            stride, rows, keys = tiling(static_level, length)
            lead = keys - rows

            @pl.when(pl.program_id(0) == 0)
            def _():
                row = lax.broadcasted_iota(jnp.int32, (rows, keys), 0)
                col = lax.broadcasted_iota(jnp.int32, (rows, keys), 1)
                distance = row - col + lead
                inside = (distance >= 0) & (distance < reach_keys)
                for block in range(length // stride // rows):
                    there = col + (block * rows - lead) + seat * (length // stride) >= 0
                    bias[block, :rows, :keys] = jnp.where(inside & there, 0.0, masked_fill)

            for number, (block, q_first, k_first) in enumerate(unit_list(static_level, length)):
                q = q_all[pl.ds(q_first, rows, stride=stride), :].astype(jnp.bfloat16)
                k = k_all[pl.ds(k_first, keys, stride=stride), :].astype(jnp.bfloat16)
                s = lax.dot_general(
                    q, k, (((1,), (1,)), ((), ())), preferred_element_type=jnp.float32
                )
                s = s + bias[block, :rows, :keys]
                peak = jnp.max(s, axis=-1, keepdims=True)
                w = jnp.exp2((s - peak) * factor)
                total = jnp.sum(w, axis=-1, keepdims=True)
                lower = number * rows
                p_ref[head, lower : lower + rows, :keys] = w.astype(jnp.bfloat16)
                t_ref[head, lower : lower + rows, :] = jnp.broadcast_to(total, (rows, HS))


def mix_kernel(length, count, first_head, parts, dilation, window, p_ref, t_ref, *rest):
    value_refs, rest = take_refs(rest, parts)
    o_ref, v_all, o_all = rest[-3:]
    place = placing(dilation, window, count)
    level = place[0]
    head = pl.program_id(0) + first_head
    spread(v_all, value_refs, place, length, head)
    for static_level in range(LEVELS):

        @pl.when(level == static_level)
        def _(static_level=static_level):
            stride, rows, keys = tiling(static_level, length)
            for number, (block, q_first, k_first) in enumerate(unit_list(static_level, length)):
                v = v_all[pl.ds(k_first, keys, stride=stride), :].astype(jnp.bfloat16)
                lower = number * rows
                p = p_ref[head, lower : lower + rows, :keys]
                mixed = jnp.dot(p, v, preferred_element_type=jnp.float32)
                mixed = mixed / t_ref[head, lower : lower + rows, :]
                o_all[pl.ds(q_first, rows, stride=stride), :] = mixed

    o_ref[...] = o_all[...].astype(jnp.bfloat16)


def routes(count):
    relay_from = [s for s in range(3, count, 4) if s + REACH < count]
    near = [(s, s + 1) for s in range(0, count - 1, 2)] + [(s, s + REACH) for s in relay_from]
    far = [(s, s + REACH) for s in range(1, count - REACH, 2) if s not in relay_from]
    two = [(s, s + 2) for s in range(count - 2) if s not in relay_from]
    relay = [(s + 3, s + 2) for s in relay_from]
    swap = [(s, s ^ 1) for s in range(2, count) if s - 2 not in relay_from]
    relay_swap = [(s + 2, s + 1) for s in relay_from]
    return near, far, two, relay, swap, relay_swap


def body(queries, key_heads, value_heads, dilation, window):
    length, width = queries.shape
    heads_here = width // HS
    count = lax.axis_size("seq")
    near, far, two, relay, swap, relay_swap = routes(count)
    key_parts = (0, 3 * heads_here // 8)
    value_parts = (0, heads_here // 2)

    def send(value, pairs):
        return lax.ppermute(value, "seq", pairs)

    def gather(value, parts):
        ends = parts[1:] + (heads_here,)
        pieces = [value[:, low * HS : high * HS] for low, high in zip(parts, ends)]
        by_two = [send(piece, two) for piece in pieces]
        nearby = send(value, near)
        beyond = send(value, far)
        relays = send(nearby, relay)
        swapped = [send(piece, swap) for piece in by_two]
        relay_swapped = send(relays, relay_swap)
        return (nearby, beyond, relays, relay_swapped, value), by_two, swapped

    whole = pl.BlockSpec(memory_space=pltpu.VMEM)
    keys_most = max(tiling(level, length)[2] for level in range(LEVELS))
    rows_all = (REACH + 1) * length
    blocks_most = max(length // tiling(l, length)[0] // tiling(l, length)[1] for l in range(LEVELS))
    rows_most = max(tiling(l, length)[1] for l in range(LEVELS))

    def call(kernel, heads, parts, operands, specs, out_specs, out_shape, scratch, **more):
        return pl.pallas_call(
            partial(kernel, length, count, heads[0], parts),
            grid_spec=pltpu.PrefetchScalarGridSpec(
                num_scalar_prefetch=2,
                grid=(heads[1] - heads[0],),
                in_specs=specs,
                out_specs=out_specs,
                scratch_shapes=scratch,
            ),
            out_shape=out_shape,
            compiler_params=pltpu.CompilerParams(
                dimension_semantics=("arbitrary",), vmem_limit_bytes=VMEM_LIMIT
            ),
            **more,
        )(dilation, window, *operands)

    def column(first_head):
        return pl.BlockSpec((length, HS), lambda h, *_: (0, h + first_head))

    keys, keys_two, keys_swap = gather(key_heads, key_parts)
    values, values_two, values_swap = gather(value_heads, value_parts)
    weights, totals = call(
        score_kernel,
        (0, heads_here),
        key_parts,
        (queries, *keys, *keys_two, *keys_swap),
        [column(0)] + [whole] * 4 + [column(0)] + [whole] * (2 * len(key_parts)),
        [whole, whole],
        [
            pltpu.VMEM((heads_here, length, keys_most), jnp.bfloat16),
            pltpu.VMEM((heads_here, length, HS), jnp.float32),
        ],
        [
            pltpu.VMEM((length, HS), jnp.float32),
            pltpu.VMEM((rows_all, HS), jnp.float32),
            pltpu.VMEM((blocks_most, rows_most, keys_most), jnp.float32),
        ],
    )
    out = ()
    for part, low in enumerate(value_parts):
        high = (value_parts + (heads_here,))[part + 1]
        operands = (weights, totals, *values, values_two[part], values_swap[part], *out)
        specs = [whole] * 6 + [column(low)] + [whole] * 2
        more = {}
        if out:
            specs = specs + [pl.BlockSpec(memory_space=pl.ANY)]
            more = dict(input_output_aliases={len(operands) + 1: 0})
        out = (
            call(
                mix_kernel,
                (low, high),
                (low,),
                operands,
                specs,
                column(low),
                jax.ShapeDtypeStruct((length, width), jnp.bfloat16),
                [pltpu.VMEM((rows_all, HS), jnp.float32), pltpu.VMEM((length, HS), jnp.float32)],
                **more,
            ),
        )
    return out[0]


def solution(mesh):
    return jax.shard_map(
        body,
        mesh=mesh,
        in_specs=(P("seq", "head"), P("seq", "head"), P("seq", "head"), P(), P()),
        out_specs=P("seq", "head"),
        check_vma=False,
    )
```

```python
from functools import partial

import jax
import jax.numpy as jnp
from jax import lax
from jax.experimental import pallas as pl
from jax.experimental.pallas import tpu as pltpu
from jax.sharding import PartitionSpec as P


HS = 128
WIN = 192
LEVELS = 4
REACH = 3
LOG2E = 1.4426950408889634
masked_fill = -1e30
VMEM_LIMIT = 40 << 20


def tiling(level, length):
    stride = 2**level
    rows = min(128, length // stride)
    keys = -(-(rows + WIN) // 128) * 128
    return (stride, rows, keys)


def unit_list(level, length):
    stride, rows, keys = tiling(level, length)
    blocks = length // stride // rows
    lead = keys - rows
    units = []
    for residue in range(stride):
        for block in range(blocks):
            first = residue + block * rows * stride
            units.append((block, first, REACH * length + first - lead * stride))
    return units


def placing(dilation, window, count):
    seat = lax.axis_index("seq")
    group = lax.axis_index("head")
    step = dilation[group]
    level = sum((step > 2**i).astype(jnp.int32) for i in range(LEVELS - 1))
    near, _, _, relay, _, relay_swap = routes(count)

    def among(targets):
        return sum([(seat == b).astype(jnp.int32) for b in targets], jnp.int32(0))

    relayed = among([b for _, b in relay])
    partner_relayed = among([b for _, b in relay_swap])
    from_near = among([b for _, b in near])
    return level, window[group], seat, lax.rem(seat, 2), relayed, partner_relayed, from_near


def spread(scratch, refs, place, length, head):
    level, _, _, odd, relayed, partner_relayed, from_near = place
    near, far, relay, relay_swapped, own, two, swap = refs

    def put(at, ref, column):
        columns = pl.ds(pl.multiple_of(column * HS, HS), HS)
        scratch[pl.ds(pl.multiple_of(at, 8), length), :] = ref[:, columns].astype(jnp.float32)

    def put_part(at, parts, wanted):
        if len(parts) == 1:
            low, ref = parts[0]

            @pl.when(wanted)
            def _():
                put(at, ref, head - low)

        else:
            (low, first), (high, second) = parts

            @pl.when(jnp.logical_and(wanted, head < high))
            def _():
                put(at, first, head - low)

            @pl.when(jnp.logical_and(wanted, head >= high))
            def _():
                put(at, second, head - high)

    put(REACH * length, own, 0)

    @pl.when(jnp.logical_and(jnp.logical_or(odd == 1, level == 3), from_near == 0))
    def _():
        put(jnp.where(odd == 1, 2 * length, 0), far, head)

    @pl.when(jnp.logical_and(level == 3, from_near == 1))
    def _():
        put(0, near, head)

    put_part(
        jnp.where(odd == 1, 0, 2 * length),
        swap,
        jnp.logical_and(jnp.logical_or(odd == 0, level == 3), partner_relayed == 0),
    )

    @pl.when(partner_relayed == 1)
    def _():
        put(2 * length, relay_swapped, head)

    put_part(length, two, jnp.logical_and(level >= 2, relayed == 0))

    @pl.when(jnp.logical_and(level >= 2, relayed == 1))
    def _():
        put(length, relay, head)


def take_refs(refs, parts):
    count = len(parts)
    two = list(zip(parts, refs[5 : 5 + count]))
    swap = list(zip(parts, refs[5 + count : 5 + 2 * count]))
    return (*refs[:5], two, swap), refs[5 + 2 * count :]


def score_kernel(length, count, first_head, parts, dilation, window, q_ref, *rest):
    key_refs, (p_ref, t_ref, q_all, k_all, bias) = take_refs(rest, parts)
    place = placing(dilation, window, count)
    level, reach_keys, seat = place[:3]
    head = pl.program_id(0) + first_head
    q_all[...] = q_ref[...].astype(jnp.float32)
    spread(k_all, key_refs, place, length, head)
    factor = HS ** (-0.5) * LOG2E
    for static_level in range(LEVELS):

        @pl.when(level == static_level)
        def _(static_level=static_level):
            stride, rows, keys = tiling(static_level, length)
            lead = keys - rows

            @pl.when(pl.program_id(0) == 0)
            def _():
                row = lax.broadcasted_iota(jnp.int32, (rows, keys), 0)
                col = lax.broadcasted_iota(jnp.int32, (rows, keys), 1)
                distance = row - col + lead
                inside = (distance >= 0) & (distance < reach_keys)
                for block in range(length // stride // rows):
                    there = col + (block * rows - lead) + seat * (length // stride) >= 0
                    bias[block, :rows, :keys] = jnp.where(inside & there, 0.0, masked_fill)

            for number, (block, q_first, k_first) in enumerate(unit_list(static_level, length)):
                q = q_all[pl.ds(q_first, rows, stride=stride), :].astype(jnp.bfloat16)
                k = k_all[pl.ds(k_first, keys, stride=stride), :].astype(jnp.bfloat16)
                s = lax.dot_general(
                    q, k, (((1,), (1,)), ((), ())), preferred_element_type=jnp.float32
                )
                s = s + bias[block, :rows, :keys]
                peak = jnp.max(s, axis=-1, keepdims=True)
                w = jnp.exp2((s - peak) * factor)
                total = jnp.sum(w, axis=-1, keepdims=True)
                lower = number * rows
                p_ref[head, lower : lower + rows, :keys] = w.astype(jnp.bfloat16)
                t_ref[head, lower : lower + rows, :] = jnp.broadcast_to(total, (rows, HS))


def mix_kernel(length, count, first_head, parts, dilation, window, p_ref, t_ref, *rest):
    value_refs, rest = take_refs(rest, parts)
    o_ref, v_all, o_all = rest[-3:]
    place = placing(dilation, window, count)
    level = place[0]
    head = pl.program_id(0) + first_head
    spread(v_all, value_refs, place, length, head)
    for static_level in range(LEVELS):

        @pl.when(level == static_level)
        def _(static_level=static_level):
            stride, rows, keys = tiling(static_level, length)
            for number, (block, q_first, k_first) in enumerate(unit_list(static_level, length)):
                v = v_all[pl.ds(k_first, keys, stride=stride), :].astype(jnp.bfloat16)
                lower = number * rows
                p = p_ref[head, lower : lower + rows, :keys]
                mixed = jnp.dot(p, v, preferred_element_type=jnp.float32)
                mixed = mixed / t_ref[head, lower : lower + rows, :]
                o_all[pl.ds(q_first, rows, stride=stride), :] = mixed

    o_ref[...] = o_all[...].astype(jnp.bfloat16)


def routes(count):
    relay_from = [s for s in range(3, count, 4) if s + REACH < count]
    near = [(s, s + REACH) for s in relay_from]
    far = [(s, s + REACH) for s in range(1, count - REACH, 2) if s not in relay_from]
    far = far + [(s, s + 1) for s in range(0, count - 1, 2)]
    two = [(s, s + 2) for s in range(count - 2) if s not in relay_from]
    relay = [(s + 3, s + 2) for s in relay_from]
    swap = [(s, s ^ 1) for s in range(2, count) if s - 2 not in relay_from]
    relay_swap = [(s + 2, s + 1) for s in relay_from]
    return near, far, two, relay, swap, relay_swap


def body(queries, key_heads, value_heads, dilation, window):
    length, width = queries.shape
    heads_here = width // HS
    count = lax.axis_size("seq")
    near, far, two, relay, swap, relay_swap = routes(count)
    key_parts = (0,)
    value_parts = (0, heads_here // 2)

    def send(value, pairs):
        return lax.ppermute(value, "seq", pairs)

    def gather(value, parts):
        ends = parts[1:] + (heads_here,)
        pieces = [value[:, low * HS : high * HS] for low, high in zip(parts, ends)]
        by_two = [send(piece, two) for piece in pieces]
        nearby = send(value, near)
        beyond = send(value, far)
        relays = send(nearby, relay)
        swapped = [send(piece, swap) for piece in by_two]
        relay_swapped = send(relays, relay_swap)
        return (nearby, beyond, relays, relay_swapped, value), by_two, swapped

    whole = pl.BlockSpec(memory_space=pltpu.VMEM)
    keys_most = max(tiling(level, length)[2] for level in range(LEVELS))
    rows_all = (REACH + 1) * length
    blocks_most = max(length // tiling(l, length)[0] // tiling(l, length)[1] for l in range(LEVELS))
    rows_most = max(tiling(l, length)[1] for l in range(LEVELS))

    def call(kernel, heads, parts, operands, specs, out_specs, out_shape, scratch, **more):
        return pl.pallas_call(
            partial(kernel, length, count, heads[0], parts),
            grid_spec=pltpu.PrefetchScalarGridSpec(
                num_scalar_prefetch=2,
                grid=(heads[1] - heads[0],),
                in_specs=specs,
                out_specs=out_specs,
                scratch_shapes=scratch,
            ),
            out_shape=out_shape,
            compiler_params=pltpu.CompilerParams(
                dimension_semantics=("arbitrary",), vmem_limit_bytes=VMEM_LIMIT
            ),
            **more,
        )(dilation, window, *operands)

    def column(first_head):
        return pl.BlockSpec((length, HS), lambda h, *_: (0, h + first_head))

    keys, keys_two, keys_swap = gather(key_heads, key_parts)
    values, values_two, values_swap = gather(value_heads, value_parts)
    weights, totals = call(
        score_kernel,
        (0, heads_here),
        key_parts,
        (queries, *keys, *keys_two, *keys_swap),
        [column(0)] + [whole] * 4 + [column(0)] + [whole] * (2 * len(key_parts)),
        [whole, whole],
        [
            pltpu.VMEM((heads_here, length, keys_most), jnp.bfloat16),
            pltpu.VMEM((heads_here, length, HS), jnp.float32),
        ],
        [
            pltpu.VMEM((length, HS), jnp.float32),
            pltpu.VMEM((rows_all, HS), jnp.float32),
            pltpu.VMEM((blocks_most, rows_most, keys_most), jnp.float32),
        ],
    )
    out = ()
    for part, low in enumerate(value_parts):
        high = (value_parts + (heads_here,))[part + 1]
        operands = (weights, totals, *values, values_two[part], values_swap[part], *out)
        specs = [whole] * 6 + [column(low)] + [whole] * 2
        more = {}
        if out:
            specs = specs + [pl.BlockSpec(memory_space=pl.ANY)]
            more = dict(input_output_aliases={len(operands) + 1: 0})
        out = (
            call(
                mix_kernel,
                (low, high),
                (low,),
                operands,
                specs,
                column(low),
                jax.ShapeDtypeStruct((length, width), jnp.bfloat16),
                [pltpu.VMEM((rows_all, HS), jnp.float32), pltpu.VMEM((length, HS), jnp.float32)],
                **more,
            ),
        )
    return out[0]


def solution(mesh):
    return jax.shard_map(
        body,
        mesh=mesh,
        in_specs=(P("seq", "head"), P("seq", "head"), P("seq", "head"), P(), P()),
        out_specs=P("seq", "head"),
        check_vma=False,
    )
```

```python
from functools import partial
from itertools import product

import jax
import jax.numpy as jnp
from jax import lax
from jax.experimental import pallas as pl
from jax.experimental.pallas import tpu as pltpu
from jax.sharding import PartitionSpec as P


HS = 128
WIN = 192
LEVELS = 4
REACH = 3
LOG2E = 1.4426950408889634
PACK = 128
SPLIT = 4
TOGETHER = 4
masked_fill = -1e30
VMEM_LIMIT = 40 << 20


def tiling(level, length):
    stride = 2**level
    rows = min(128, length // stride)
    keys = -(-(rows + WIN) // 128) * 128
    return (stride, rows, keys)


def unit_list(level, length):
    stride, rows, _ = tiling(level, length)
    blocks = length // stride // rows
    return [(residue, block) for residue in range(stride) for block in range(blocks)]


def class_pieces(level, length, residue, block):
    stride, rows, keys = tiling(level, length)
    per = length // stride
    low = REACH * per + block * rows + rows - keys
    high = low + keys
    pieces = []
    for region in range(REACH + 1):
        start, stop = max(low, region * per), min(high, (region + 1) * per)
        if start < stop:
            pieces.append((region, residue * per + start - region * per, stop - start))
    return pieces


def routes(count, both):
    relay_from = [s for s in range(3, count, 4) if s + REACH < count]
    through = [s for s in relay_from] + [s - 1 for s in relay_from if both]
    near = [(s, s + REACH) for s in relay_from]
    relay = [(s + 3, s + 2) for s in relay_from]
    relay_swap = [(s + 2, s + 1) for s in relay_from]
    if both:
        near = near + [(s - 1, s + 4) for s in relay_from]
        relay = relay + [(s + 4, s + 1) for s in relay_from]
        relay_swap = relay_swap + [(s + 1, s + 2) for s in relay_from]
    two = [(s, s + 2) for s in range(count - 2) if s not in through]
    swap = [(s, s ^ 1) for s in range(2, count) if s - 2 not in through]
    far = [(s, s + REACH) for s in range(1, count - REACH, 2) if s not in relay_from]
    far = far + [(s, s + 1) for s in range(0, count - 1, 2)]
    return dict(near=near, far=far, two=two, relay=relay, swap=swap, rswap=relay_swap)


def level_of(dilation):
    step = dilation[lax.axis_index("head")]
    return sum((step > 2**i).astype(jnp.int32) for i in range(LEVELS - 1))


def spread(scratch, refs, level, length, count, both, columns):
    near, far, relay, relay_swapped, two, swapped = refs
    seat = lax.axis_index("seq")
    odd = lax.rem(seat, 2)
    plan = routes(count, both)

    def among(targets):
        return sum([(seat == b).astype(jnp.int32) for b in targets], jnp.int32(0))

    from_near = among([a + REACH for a, b in plan["near"] if b == a + REACH])
    from_relay = among([b for _, b in plan["relay"]])
    from_relay_swap = among([b for _, b in plan["rswap"]])

    def put(at, ref, first):
        for i in range(TOGETHER):
            part = ref[:, pl.ds(pl.multiple_of((first + i) * HS, HS), HS)]
            rows = pl.ds(pl.multiple_of(at, length), length)
            scratch[i, rows, :] = part.astype(scratch.dtype)

    all_of = jnp.logical_and
    far_wanted = all_of(jnp.logical_or(odd == 1, level == 3), from_near == 0)
    swap_wanted = jnp.logical_or(odd == 0, level == 3)
    swap_at = jnp.where(odd == 1, 0, 2 * length)
    for wanted, at, ref, column in (
        (far_wanted, jnp.where(odd == 1, 2 * length, 0), far, columns[0]),
        (all_of(level == 3, from_near == 1), 0, near, columns[1]),
        (all_of(swap_wanted, from_relay_swap == 0), swap_at, swapped, columns[1]),
        (all_of(swap_wanted, from_relay_swap == 1), swap_at, relay_swapped, columns[1]),
        (all_of(level >= 2, from_relay == 0), length, two, columns[1]),
        (all_of(level >= 2, from_relay == 1), length, relay, columns[1]),
    ):

        @pl.when(wanted)
        def _(at=at, ref=ref, column=column):
            put(at, ref, column)


def class_kernel(length, splits, dilation, *rest):
    inputs = len(splits)
    in_refs, rest = rest[:inputs], rest[inputs:]
    scratch = rest[-1]
    out_refs = rest[:-1]
    level = level_of(dilation)
    block = pl.program_id(0)
    heads = in_refs[0].shape[1] // HS
    at_out = 0
    for ref, parts in zip(in_refs, splits):
        outs = out_refs[at_out : at_out + len(parts)]
        at_out += len(parts)
        for head in range(heads):
            scratch[head] = ref[:, head * HS : (head + 1) * HS].astype(jnp.float32)
        for static_level in range(LEVELS):

            @pl.when(level == static_level)
            def _(static_level=static_level, outs=outs, parts=parts):
                stride = 2**static_level
                rows = PACK // stride
                for head in range(heads):
                    for residue in range(stride):
                        piece = scratch[head, pl.ds(residue, rows, stride=stride), :]
                        piece = piece.astype(jnp.bfloat16)
                        at = pl.multiple_of(residue * (length // stride) + block * rows, rows)
                        for out, (low, high) in zip(outs, parts):
                            if low <= head < high:
                                lane = (head - low) * HS
                                out[pl.ds(at, rows), lane : lane + HS] = piece


def score_kernel(length, count, dilation, window, q_ref, own_ref, *rest):
    key_refs, (p_ref, t_ref, k_all, bias) = rest[:6], rest[6:]
    level = level_of(dilation)
    seat = lax.axis_index("seq")
    reach_keys = window[lax.axis_index("head")]
    first = pl.program_id(0) * TOGETHER
    spread(k_all, key_refs, level, length, count, False, (first, first))
    factor = HS ** (-0.5) * LOG2E
    for static_level in range(LEVELS):

        @pl.when(level == static_level)
        def _(static_level=static_level):
            stride, rows, keys = tiling(static_level, length)
            lead = keys - rows

            @pl.when(first == 0)
            def _():
                row = lax.broadcasted_iota(jnp.int32, (rows, keys), 0)
                col = lax.broadcasted_iota(jnp.int32, (rows, keys), 1)
                distance = row - col + lead
                inside = (distance >= 0) & (distance < reach_keys)
                for block in range(length // stride // rows):
                    there = col + (block * rows - lead) + seat * (length // stride) >= 0
                    bias[block, :rows, :keys] = jnp.where(inside & there, 0.0, masked_fill)

            units = enumerate(unit_list(static_level, length))
            for (number, (residue, block)), i in product(units, range(TOGETHER)):
                head = first + i
                lanes = pl.ds(pl.multiple_of(head * HS, HS), HS)
                lower = number * rows
                parts = []
                earlier = max(0, lead - block * rows)
                if earlier:
                    at = REACH * length + residue - earlier * stride
                    parts.append(
                        k_all[i, pl.ds(at, earlier, stride=stride), :].astype(jnp.bfloat16)
                    )
                _, start, size = class_pieces(static_level, length, residue, block)[-1]
                parts.append(own_ref[start : start + size, lanes])
                k = jnp.concatenate(parts, axis=0) if len(parts) > 1 else parts[0]
                s = lax.dot_general(
                    q_ref[lower : lower + rows, lanes],
                    k,
                    (((1,), (1,)), ((), ())),
                    preferred_element_type=jnp.float32,
                )
                s = s + bias[block, :rows, :keys]
                peak = jnp.max(s, axis=-1, keepdims=True)
                w = jnp.exp2((s - peak) * factor)
                total = jnp.sum(w, axis=-1, keepdims=True)
                p_ref[head, lower : lower + rows, :keys] = w.astype(jnp.bfloat16)
                t_ref[head, lower : lower + rows, :] = jnp.broadcast_to(1.0 / total, (rows, HS))


def mix_kernel(length, count, first_head, both, dilation, p_ref, t_ref, own_ref, *rest):
    value_refs, rest = rest[:6], rest[6:]
    o_ref, v_all, o_all, o_out, sems = rest[-5:]
    level = level_of(dilation)
    step = pl.program_id(0) * TOGETHER
    spread(v_all, value_refs, level, length, count, both, (step + first_head, step))
    for static_level in range(LEVELS):

        @pl.when(level == static_level)
        def _(static_level=static_level):
            stride, rows, keys = tiling(static_level, length)
            units = enumerate(unit_list(static_level, length))
            for (number, (residue, block)), i in product(units, range(TOGETHER)):
                head = first_head + step + i
                lanes = pl.ds(pl.multiple_of(head * HS, HS), HS)
                lower = number * rows
                parts = []
                for region, start, size in class_pieces(static_level, length, residue, block):
                    if region == REACH:
                        parts.append(own_ref[start : start + size, lanes])
                    else:
                        start = region * length + start
                        parts.append(v_all[i, start : start + size, :])
                v = jnp.concatenate(parts, axis=0) if len(parts) > 1 else parts[0]
                p = p_ref[head, lower : lower + rows, :keys]
                mixed = jnp.dot(p, v, preferred_element_type=jnp.float32)
                mixed = mixed * t_ref[head, lower : lower + rows, :]
                at = residue + block * rows * stride
                o_all[i, pl.ds(at, rows, stride=stride), :] = mixed

    def copy_of(at):
        lanes = pl.ds(pl.multiple_of((at + first_head) * HS, HS), HS)
        return pltpu.make_async_copy(o_out.at[at], o_ref.at[:, lanes], sems.at[at])

    for i in range(TOGETHER):
        o_out[step + i] = o_all[i].astype(jnp.bfloat16)
        copy_of(step + i).start()

    @pl.when(pl.program_id(0) == pl.num_programs(0) - 1)
    def _():
        for at in range(o_out.shape[0]):
            copy_of(at).wait()


def body(queries, key_heads, value_heads, dilation, window):
    length, width = queries.shape
    heads_here = width // HS
    count = lax.axis_size("seq")
    bounds = (0, SPLIT * heads_here // 8, heads_here)
    whole = pl.BlockSpec(memory_space=pltpu.VMEM)

    def in_hbm(value):
        return pltpu.with_memory_space_constraint(value, pltpu.HBM)

    def send(name, value, both=False):
        return lax.ppermute(value, "seq", routes(count, both)[name.split("_")[0]])

    def call(kernel, steps, scalars, operands, specs, out_specs, out_shape, scratch, **more):
        return pl.pallas_call(
            kernel,
            grid_spec=pltpu.PrefetchScalarGridSpec(
                num_scalar_prefetch=len(scalars),
                grid=(steps,),
                in_specs=specs,
                out_specs=out_specs,
                scratch_shapes=scratch,
            ),
            out_shape=out_shape,
            compiler_params=pltpu.CompilerParams(
                dimension_semantics=("arbitrary",), vmem_limit_bytes=VMEM_LIMIT
            ),
            **more,
        )(*[pltpu.with_memory_space_constraint(scalar, pltpu.SMEM) for scalar in scalars], *operands)

    def by_class(arrays, splits):
        shapes = [
            pltpu.VMEM((length, (high - low) * HS), jnp.bfloat16)
            for parts in splits
            for low, high in parts
        ]
        return call(
            partial(class_kernel, length, splits),
            length // PACK,
            (dilation,),
            [in_hbm(array) for array in arrays],
            [pl.BlockSpec((PACK, width), lambda i, *_: (i, 0))] * len(arrays),
            [whole] * len(shapes),
            shapes,
            [pltpu.VMEM((heads_here, PACK, HS), jnp.float32)],
        )

    keys_most = max(tiling(level, length)[2] for level in range(LEVELS))
    blocks_most = max(length // tiling(l, length)[0] // tiling(l, length)[1] for l in range(LEVELS))
    rows_most = max(tiling(l, length)[1] for l in range(LEVELS))

    two_k = send("two_k", key_heads)
    near_k = send("near_k", key_heads)
    far_k = send("far_k", key_heads)
    relay_k = send("relay_k", near_k)
    keys = (near_k, far_k, relay_k, send("rswap_k", relay_k), two_k, send("swap_k", two_k))

    everything = (0, heads_here)
    own_v, *own_parts = by_class([value_heads], ((everything, bounds[:2], bounds[1:]),))
    far_v = send("far_v", own_v)
    values = []
    for i, part in enumerate(own_parts):
        both = i == 1
        two_v = send(f"two_v{i}", part, both)
        near_v = send(f"near_v{i}", part, both)
        relay_v = send(f"relay_v{i}", near_v, both)
        values.append(
            (
                near_v,
                far_v,
                relay_v,
                send(f"rswap_v{i}", relay_v, both),
                two_v,
                send(f"swap_v{i}", two_v, both),
            )
        )

    class_q, own_k = by_class([queries, key_heads], ((everything,), (everything,)))
    weights, totals = call(
        partial(score_kernel, length, count),
        heads_here // TOGETHER,
        (dilation, window),
        (class_q, own_k, *keys),
        [whole] * 8,
        [whole, whole],
        [
            pltpu.VMEM((heads_here, length, keys_most), jnp.bfloat16),
            pltpu.VMEM((heads_here, length, HS), jnp.float32),
        ],
        [
            pltpu.VMEM((TOGETHER, REACH * length, HS), jnp.float32),
            pltpu.VMEM((blocks_most, rows_most, keys_most), jnp.float32),
        ],
    )
    out = ()
    for i in range(2):
        specs, more = [whole] * 9, {}
        if out:
            specs = specs + [pl.BlockSpec(memory_space=pl.ANY)]
            more = dict(input_output_aliases={10: 0})
        out = (
            call(
                partial(mix_kernel, length, count, bounds[i], i == 1),
                (bounds[i + 1] - bounds[i]) // TOGETHER,
                (dilation,),
                (weights, totals, own_v, *values[i], *out),
                specs,
                pl.BlockSpec(memory_space=pl.ANY),
                jax.ShapeDtypeStruct((length, width), jnp.bfloat16),
                [
                    pltpu.VMEM((TOGETHER, REACH * length, HS), jnp.bfloat16),
                    pltpu.VMEM((TOGETHER, length, HS), jnp.float32),
                    pltpu.VMEM((bounds[i + 1] - bounds[i], length, HS), jnp.bfloat16),
                    pltpu.SemaphoreType.DMA((bounds[i + 1] - bounds[i],)),
                ],
                **more,
            ),
        )
    return out[0]


def solution(mesh):
    return jax.shard_map(
        body,
        mesh=mesh,
        in_specs=(P("seq", "head"), P("seq", "head"), P("seq", "head"), P(), P()),
        out_specs=P("seq", "head"),
        check_vma=False,
    )
```

```python
from functools import partial
from itertools import product

import jax
import jax.numpy as jnp
from jax import lax
from jax.experimental import pallas as pl
from jax.experimental.pallas import tpu as pltpu
from jax.sharding import PartitionSpec as P


HS = 128
WIN = 192
LEVELS = 4
REACH = 3
LOG2E = 1.4426950408889634
PACK = 128
SPLIT = 5
TOGETHER = 8
MIX_TOGETHER = (5, 3)
masked_fill = -1e30
VMEM_LIMIT = 40 << 20


def tiling(level, length):
    stride = 2**level
    rows = min(128, length // stride)
    keys = -(-(rows + WIN) // 128) * 128
    return (stride, rows, keys)


def unit_list(level, length):
    stride, rows, _ = tiling(level, length)
    blocks = length // stride // rows
    return [(residue, block) for residue in range(stride) for block in range(blocks)]


def class_pieces(level, length, residue, block):
    stride, rows, keys = tiling(level, length)
    per = length // stride
    low = REACH * per + block * rows + rows - keys
    high = low + keys
    pieces = []
    for region in range(REACH + 1):
        start, stop = max(low, region * per), min(high, (region + 1) * per)
        if start < stop:
            pieces.append((region, residue * per + start - region * per, stop - start))
    return pieces


def routes(count, both):
    relay_from = [s for s in range(3, count, 4) if s + REACH < count]
    through = [s for s in relay_from] + [s - 1 for s in relay_from if both]
    near = [(s, s + REACH) for s in relay_from]
    relay = [(s + 3, s + 2) for s in relay_from]
    relay_swap = [(s + 2, s + 1) for s in relay_from]
    if both:
        near = near + [(s - 1, s + 4) for s in relay_from]
        relay = relay + [(s + 4, s + 1) for s in relay_from]
        relay_swap = relay_swap + [(s + 1, s + 2) for s in relay_from]
    two = [(s, s + 2) for s in range(count - 2) if s not in through]
    swap = [(s, s ^ 1) for s in range(2, count) if s - 2 not in through]
    far = [(s, s + REACH) for s in range(1, count - REACH, 2) if s not in relay_from]
    far = far + [(s, s + 1) for s in range(0, count - 1, 2)]
    return dict(near=near, far=far, two=two, relay=relay, swap=swap, rswap=relay_swap)


def level_of(dilation):
    step = dilation[lax.axis_index("head")]
    return sum((step > 2**i).astype(jnp.int32) for i in range(LEVELS - 1))


def spread(scratch, refs, level, length, count, both, columns):
    near, far, relay, relay_swapped, two, swapped = refs
    seat = lax.axis_index("seq")
    odd = lax.rem(seat, 2)
    plan = routes(count, both)

    def among(targets):
        return sum([(seat == b).astype(jnp.int32) for b in targets], jnp.int32(0))

    from_near = among([a + REACH for a, b in plan["near"] if b == a + REACH])
    from_relay = among([b for _, b in plan["relay"]])
    from_relay_swap = among([b for _, b in plan["rswap"]])

    def put(at, ref, first):
        for i in range(scratch.shape[0]):
            part = ref[:, pl.ds(pl.multiple_of((first + i) * HS, HS), HS)]
            rows = pl.ds(pl.multiple_of(at, length), length)
            scratch[i, rows, :] = part.astype(scratch.dtype)

    all_of = jnp.logical_and
    far_wanted = all_of(jnp.logical_or(odd == 1, level == 3), from_near == 0)
    swap_wanted = jnp.logical_or(odd == 0, level == 3)
    swap_at = jnp.where(odd == 1, 0, 2 * length)
    for wanted, at, ref, column in (
        (far_wanted, jnp.where(odd == 1, 2 * length, 0), far, columns[0]),
        (all_of(level == 3, from_near == 1), 0, near, columns[1]),
        (all_of(swap_wanted, from_relay_swap == 0), swap_at, swapped, columns[1]),
        (all_of(swap_wanted, from_relay_swap == 1), swap_at, relay_swapped, columns[1]),
        (all_of(level >= 2, from_relay == 0), length, two, columns[1]),
        (all_of(level >= 2, from_relay == 1), length, relay, columns[1]),
    ):

        @pl.when(wanted)
        def _(at=at, ref=ref, column=column):
            put(at, ref, column)


def class_kernel(length, splits, dilation, *rest):
    inputs = len(splits)
    in_refs, rest = rest[:inputs], rest[inputs:]
    scratch = rest[-1]
    out_refs = rest[:-1]
    level = level_of(dilation)
    block = pl.program_id(0)
    heads = in_refs[0].shape[1] // HS
    at_out = 0
    for ref, parts in zip(in_refs, splits):
        outs = out_refs[at_out : at_out + len(parts)]
        at_out += len(parts)
        for head in range(heads):
            scratch[head] = ref[:, head * HS : (head + 1) * HS].astype(jnp.float32)
        for static_level in range(LEVELS):

            @pl.when(level == static_level)
            def _(static_level=static_level, outs=outs, parts=parts):
                stride = 2**static_level
                rows = PACK // stride
                for head in range(heads):
                    for residue in range(stride):
                        piece = scratch[head, pl.ds(residue, rows, stride=stride), :]
                        piece = piece.astype(jnp.bfloat16)
                        at = pl.multiple_of(residue * (length // stride) + block * rows, rows)
                        for out, (low, high) in zip(outs, parts):
                            if low <= head < high:
                                lane = (head - low) * HS
                                out[pl.ds(at, rows), lane : lane + HS] = piece


def score_kernel(length, count, dilation, window, q_ref, own_ref, *rest):
    key_refs, (p_ref, t_ref, k_all, bias) = rest[:6], rest[6:]
    level = level_of(dilation)
    seat = lax.axis_index("seq")
    reach_keys = window[lax.axis_index("head")]
    first = pl.program_id(0) * TOGETHER
    spread(k_all, key_refs, level, length, count, False, (first, first))
    factor = HS ** (-0.5) * LOG2E
    for static_level in range(LEVELS):

        @pl.when(level == static_level)
        def _(static_level=static_level):
            stride, rows, keys = tiling(static_level, length)
            lead = keys - rows

            @pl.when(first == 0)
            def _():
                row = lax.broadcasted_iota(jnp.int32, (rows, keys), 0)
                col = lax.broadcasted_iota(jnp.int32, (rows, keys), 1)
                distance = row - col + lead
                inside = (distance >= 0) & (distance < reach_keys)
                for block in range(length // stride // rows):
                    there = col + (block * rows - lead) + seat * (length // stride) >= 0
                    bias[block, :rows, :keys] = jnp.where(inside & there, 0.0, masked_fill)

            units = enumerate(unit_list(static_level, length))
            for (number, (residue, block)), i in product(units, range(TOGETHER)):
                head = first + i
                lanes = pl.ds(pl.multiple_of(head * HS, HS), HS)
                lower = number * rows
                parts = []
                earlier = max(0, lead - block * rows)
                if earlier:
                    at = REACH * length + residue - earlier * stride
                    parts.append(
                        k_all[i, pl.ds(at, earlier, stride=stride), :].astype(jnp.bfloat16)
                    )
                _, start, size = class_pieces(static_level, length, residue, block)[-1]
                parts.append(own_ref[start : start + size, lanes])
                k = jnp.concatenate(parts, axis=0) if len(parts) > 1 else parts[0]
                s = lax.dot_general(
                    q_ref[lower : lower + rows, lanes],
                    k,
                    (((1,), (1,)), ((), ())),
                    preferred_element_type=jnp.float32,
                )
                s = s + bias[block, :rows, :keys]
                peak = jnp.max(s, axis=-1, keepdims=True)
                w = jnp.exp2((s - peak) * factor)
                total = jnp.sum(w, axis=-1, keepdims=True)
                p_ref[head, lower : lower + rows, :keys] = w.astype(jnp.bfloat16)
                t_ref[head, lower : lower + rows, :] = jnp.broadcast_to(1.0 / total, (rows, HS))


def mix_kernel(length, count, first_head, both, dilation, p_ref, t_ref, own_ref, *rest):
    value_refs, rest = rest[:6], rest[6:]
    o_ref, v_all, o_all, o_out, sems = rest[-5:]
    level = level_of(dilation)
    together = o_all.shape[0]
    step = pl.program_id(0) * together
    spread(v_all, value_refs, level, length, count, both, (step + first_head, step))
    for static_level in range(LEVELS):

        @pl.when(level == static_level)
        def _(static_level=static_level):
            stride, rows, keys = tiling(static_level, length)
            units = enumerate(unit_list(static_level, length))
            for (number, (residue, block)), i in product(units, range(together)):
                head = first_head + step + i
                lanes = pl.ds(pl.multiple_of(head * HS, HS), HS)
                lower = number * rows
                parts = []
                for region, start, size in class_pieces(static_level, length, residue, block):
                    if region == REACH:
                        parts.append(own_ref[start : start + size, lanes])
                    else:
                        start = region * length + start
                        parts.append(v_all[i, start : start + size, :])
                v = jnp.concatenate(parts, axis=0) if len(parts) > 1 else parts[0]
                p = p_ref[head, lower : lower + rows, :keys]
                mixed = jnp.dot(p, v, preferred_element_type=jnp.float32)
                mixed = mixed * t_ref[head, lower : lower + rows, :]
                at = residue + block * rows * stride
                o_all[i, pl.ds(at, rows, stride=stride), :] = mixed

    def copy_of(at):
        lanes = pl.ds(pl.multiple_of((at + first_head) * HS, HS), HS)
        return pltpu.make_async_copy(o_out.at[at], o_ref.at[:, lanes], sems.at[at])

    for i in range(together):
        o_out[step + i] = o_all[i].astype(jnp.bfloat16)
        copy_of(step + i).start()

    @pl.when(pl.program_id(0) == pl.num_programs(0) - 1)
    def _():
        for at in range(o_out.shape[0]):
            copy_of(at).wait()


def body(queries, key_heads, value_heads, dilation, window):
    length, width = queries.shape
    heads_here = width // HS
    count = lax.axis_size("seq")
    bounds = (0, SPLIT * heads_here // 8, heads_here)
    whole = pl.BlockSpec(memory_space=pltpu.VMEM)

    def in_hbm(value):
        return pltpu.with_memory_space_constraint(value, pltpu.HBM)

    def send(name, value, both=False):
        return lax.ppermute(value, "seq", routes(count, both)[name.split("_")[0]])

    def call(kernel, steps, scalars, operands, specs, out_specs, out_shape, scratch, **more):
        return pl.pallas_call(
            kernel,
            grid_spec=pltpu.PrefetchScalarGridSpec(
                num_scalar_prefetch=len(scalars),
                grid=(steps,),
                in_specs=specs,
                out_specs=out_specs,
                scratch_shapes=scratch,
            ),
            out_shape=out_shape,
            compiler_params=pltpu.CompilerParams(
                dimension_semantics=("arbitrary",), vmem_limit_bytes=VMEM_LIMIT
            ),
            **more,
        )(*[pltpu.with_memory_space_constraint(scalar, pltpu.SMEM) for scalar in scalars], *operands)

    def by_class(arrays, splits):
        shapes = [
            pltpu.VMEM((length, (high - low) * HS), jnp.bfloat16)
            for parts in splits
            for low, high in parts
        ]
        return call(
            partial(class_kernel, length, splits),
            length // PACK,
            (dilation,),
            [in_hbm(array) for array in arrays],
            [pl.BlockSpec((PACK, width), lambda i, *_: (i, 0))] * len(arrays),
            [whole] * len(shapes),
            shapes,
            [pltpu.VMEM((heads_here, PACK, HS), jnp.float32)],
        )

    keys_most = max(tiling(level, length)[2] for level in range(LEVELS))
    blocks_most = max(length // tiling(l, length)[0] // tiling(l, length)[1] for l in range(LEVELS))
    rows_most = max(tiling(l, length)[1] for l in range(LEVELS))

    two_k = send("two_k", key_heads)
    near_k = send("near_k", key_heads)
    far_k = send("far_k", key_heads)
    relay_k = send("relay_k", near_k)
    keys = (near_k, far_k, relay_k, send("rswap_k", relay_k), two_k, send("swap_k", two_k))

    everything = (0, heads_here)
    own_v, *own_parts = by_class([value_heads], ((everything, bounds[:2], bounds[1:]),))
    far_v = send("far_v", own_v)
    values = []
    for i, part in enumerate(own_parts):
        both = i == 1
        two_v = send(f"two_v{i}", part, both)
        near_v = send(f"near_v{i}", part, both)
        relay_v = send(f"relay_v{i}", near_v, both)
        values.append(
            (
                near_v,
                far_v,
                relay_v,
                send(f"rswap_v{i}", relay_v, both),
                two_v,
                send(f"swap_v{i}", two_v, both),
            )
        )

    class_q, own_k = by_class([queries, key_heads], ((everything,), (everything,)))
    weights, totals = call(
        partial(score_kernel, length, count),
        heads_here // TOGETHER,
        (dilation, window),
        (class_q, own_k, *keys),
        [whole] * 8,
        [whole, whole],
        [
            pltpu.VMEM((heads_here, length, keys_most), jnp.bfloat16),
            pltpu.VMEM((heads_here, length, HS), jnp.float32),
        ],
        [
            pltpu.VMEM((TOGETHER, REACH * length, HS), jnp.float32),
            pltpu.VMEM((blocks_most, rows_most, keys_most), jnp.float32),
        ],
    )
    out = ()
    for i in range(2):
        specs, more = [whole] * 9, {}
        if out:
            specs = specs + [pl.BlockSpec(memory_space=pl.ANY)]
            more = dict(input_output_aliases={10: 0})
        out = (
            call(
                partial(mix_kernel, length, count, bounds[i], i == 1),
                (bounds[i + 1] - bounds[i]) // MIX_TOGETHER[i],
                (dilation,),
                (weights, totals, own_v, *values[i], *out),
                specs,
                pl.BlockSpec(memory_space=pl.ANY),
                jax.ShapeDtypeStruct((length, width), jnp.bfloat16),
                [
                    pltpu.VMEM((MIX_TOGETHER[i], REACH * length, HS), jnp.bfloat16),
                    pltpu.VMEM((MIX_TOGETHER[i], length, HS), jnp.float32),
                    pltpu.VMEM((bounds[i + 1] - bounds[i], length, HS), jnp.bfloat16),
                    pltpu.SemaphoreType.DMA((bounds[i + 1] - bounds[i],)),
                ],
                **more,
            ),
        )
    return out[0]


def solution(mesh):
    return jax.shard_map(
        body,
        mesh=mesh,
        in_specs=(P("seq", "head"), P("seq", "head"), P("seq", "head"), P(), P()),
        out_specs=P("seq", "head"),
        check_vma=False,
    )
```

```python
from functools import partial
from itertools import product

import jax
import jax.numpy as jnp
from jax import lax
from jax.experimental import pallas as pl
from jax.experimental.pallas import tpu as pltpu
from jax.sharding import PartitionSpec as P


HS = 128
WIN = 192
LEVELS = 4
REACH = 3
LOG2E = 1.4426950408889634
PACK = 128
SPLIT = 5 / 8
masked_fill = -1e30
VMEM_LIMIT = 40 << 20


def tiling(level, length):
    stride = 2**level
    rows = min(128, length // stride)
    keys = -(-(rows + WIN) // 128) * 128
    return (stride, rows, keys)


def unit_list(level, length):
    stride, rows, _ = tiling(level, length)
    blocks = length // stride // rows
    return [(residue, block) for residue in range(stride) for block in range(blocks)]


def class_pieces(level, length, residue, block):
    stride, rows, keys = tiling(level, length)
    per = length // stride
    low = REACH * per + block * rows + rows - keys
    high = low + keys
    pieces = []
    for region in range(REACH + 1):
        start, stop = max(low, region * per), min(high, (region + 1) * per)
        if start < stop:
            pieces.append((region, residue * per + start - region * per, stop - start))
    return pieces


def routes(count, both):
    relay_from = [s for s in range(3, count, 4) if s + REACH < count]
    through = [s for s in relay_from] + [s - 1 for s in relay_from if both]
    near = [(s, s + REACH) for s in relay_from]
    relay = [(s + 3, s + 2) for s in relay_from]
    relay_swap = [(s + 2, s + 1) for s in relay_from]
    if both:
        near = near + [(s - 1, s + 4) for s in relay_from]
        relay = relay + [(s + 4, s + 1) for s in relay_from]
        relay_swap = relay_swap + [(s + 1, s + 2) for s in relay_from]
    two = [(s, s + 2) for s in range(count - 2) if s not in through]
    swap = [(s, s ^ 1) for s in range(2, count) if s - 2 not in through]
    far = [(s, s + REACH) for s in range(1, count - REACH, 2) if s not in relay_from]
    far = far + [(s, s + 1) for s in range(0, count - 1, 2)]
    return dict(near=near, far=far, two=two, relay=relay, swap=swap, rswap=relay_swap)


def level_of(dilation):
    step = dilation[lax.axis_index("head")]
    return sum((step > 2**i).astype(jnp.int32) for i in range(LEVELS - 1))


def spread(scratch, refs, level, length, count, both, columns):
    near, far, relay, relay_swapped, two, swapped = refs
    seat = lax.axis_index("seq")
    odd = lax.rem(seat, 2)
    plan = routes(count, both)

    def among(targets):
        return sum([(seat == b).astype(jnp.int32) for b in targets], jnp.int32(0))

    from_near = among([a + REACH for a, b in plan["near"] if b == a + REACH])
    from_relay = among([b for _, b in plan["relay"]])
    from_relay_swap = among([b for _, b in plan["rswap"]])

    def put(at, ref, first):
        for i in range(scratch.shape[0]):
            part = ref[:, pl.ds(pl.multiple_of((first + i) * HS, HS), HS)]
            rows = pl.ds(pl.multiple_of(at, length), length)
            scratch[i, rows, :] = part.astype(scratch.dtype)

    all_of = jnp.logical_and
    far_wanted = all_of(jnp.logical_or(odd == 1, level == 3), from_near == 0)
    swap_wanted = jnp.logical_or(odd == 0, level == 3)
    swap_at = jnp.where(odd == 1, 0, 2 * length)
    for wanted, at, ref, column in (
        (far_wanted, jnp.where(odd == 1, 2 * length, 0), far, columns[0]),
        (all_of(level == 3, from_near == 1), 0, near, columns[1]),
        (all_of(swap_wanted, from_relay_swap == 0), swap_at, swapped, columns[1]),
        (all_of(swap_wanted, from_relay_swap == 1), swap_at, relay_swapped, columns[1]),
        (all_of(level >= 2, from_relay == 0), length, two, columns[1]),
        (all_of(level >= 2, from_relay == 1), length, relay, columns[1]),
    ):

        @pl.when(wanted)
        def _(at=at, ref=ref, column=column):
            put(at, ref, column)


def class_kernel(length, splits, dilation, *rest):
    inputs = len(splits)
    in_refs, rest = rest[:inputs], rest[inputs:]
    scratch = rest[-1]
    out_refs = rest[:-1]
    level = level_of(dilation)
    block = pl.program_id(0)
    heads = in_refs[0].shape[1] // HS
    at_out = 0
    for ref, parts in zip(in_refs, splits):
        outs = out_refs[at_out : at_out + len(parts)]
        at_out += len(parts)
        for head in range(heads):
            scratch[head] = ref[:, head * HS : (head + 1) * HS].astype(jnp.float32)
        for static_level in range(LEVELS):

            @pl.when(level == static_level)
            def _(static_level=static_level, outs=outs, parts=parts):
                stride = 2**static_level
                rows = PACK // stride
                for head in range(heads):
                    for residue in range(stride):
                        piece = scratch[head, pl.ds(residue, rows, stride=stride), :]
                        piece = piece.astype(jnp.bfloat16)
                        at = pl.multiple_of(residue * (length // stride) + block * rows, rows)
                        for out, (low, high) in zip(outs, parts):
                            if low <= head < high:
                                lane = (head - low) * HS
                                out[pl.ds(at, rows), lane : lane + HS] = piece


def score_kernel(length, count, dilation, window, q_ref, own_ref, *rest):
    key_refs, (p_ref, t_ref, k_all, bias) = rest[:6], rest[6:]
    level = level_of(dilation)
    seat = lax.axis_index("seq")
    reach_keys = window[lax.axis_index("head")]
    together = k_all.shape[0]
    first = pl.program_id(0) * together
    spread(k_all, key_refs, level, length, count, False, (first, first))
    factor = HS ** (-0.5) * LOG2E
    for static_level in range(LEVELS):

        @pl.when(level == static_level)
        def _(static_level=static_level):
            stride, rows, keys = tiling(static_level, length)
            lead = keys - rows

            @pl.when(first == 0)
            def _():
                row = lax.broadcasted_iota(jnp.int32, (rows, keys), 0)
                col = lax.broadcasted_iota(jnp.int32, (rows, keys), 1)
                distance = row - col + lead
                inside = (distance >= 0) & (distance < reach_keys)
                for block in range(length // stride // rows):
                    there = col + (block * rows - lead) + seat * (length // stride) >= 0
                    bias[block, :rows, :keys] = jnp.where(inside & there, 0.0, masked_fill)

            units = enumerate(unit_list(static_level, length))
            for (number, (residue, block)), i in product(units, range(together)):
                head = first + i
                lanes = pl.ds(pl.multiple_of(head * HS, HS), HS)
                lower = number * rows
                parts = []
                earlier = max(0, lead - block * rows)
                if earlier:
                    at = REACH * length + residue - earlier * stride
                    parts.append(
                        k_all[i, pl.ds(at, earlier, stride=stride), :].astype(jnp.bfloat16)
                    )
                _, start, size = class_pieces(static_level, length, residue, block)[-1]
                parts.append(own_ref[start : start + size, lanes])
                k = jnp.concatenate(parts, axis=0) if len(parts) > 1 else parts[0]
                s = lax.dot_general(
                    q_ref[lower : lower + rows, lanes],
                    k,
                    (((1,), (1,)), ((), ())),
                    preferred_element_type=jnp.float32,
                )
                s = s + bias[block, :rows, :keys]
                peak = jnp.max(s, axis=-1, keepdims=True)
                w = jnp.exp2((s - peak) * factor)
                total = jnp.sum(w, axis=-1, keepdims=True)
                p_ref[head, lower : lower + rows, :keys] = w.astype(jnp.bfloat16)
                t_ref[head, lower : lower + rows, :] = jnp.broadcast_to(1.0 / total, (rows, HS))


def mix_kernel(length, count, first_head, both, dilation, p_ref, t_ref, own_ref, *rest):
    value_refs, rest = rest[:6], rest[6:]
    o_ref, v_all, o_all, o_out, sems = rest[-5:]
    level = level_of(dilation)
    together = o_all.shape[0]
    step = pl.program_id(0) * together
    spread(v_all, value_refs, level, length, count, both, (step + first_head, step))
    for static_level in range(LEVELS):

        @pl.when(level == static_level)
        def _(static_level=static_level):
            stride, rows, keys = tiling(static_level, length)
            units = enumerate(unit_list(static_level, length))
            for (number, (residue, block)), i in product(units, range(together)):
                head = first_head + step + i
                lanes = pl.ds(pl.multiple_of(head * HS, HS), HS)
                lower = number * rows
                parts = []
                for region, start, size in class_pieces(static_level, length, residue, block):
                    if region == REACH:
                        parts.append(own_ref[start : start + size, lanes])
                    else:
                        start = region * length + start
                        parts.append(v_all[i, start : start + size, :])
                v = jnp.concatenate(parts, axis=0) if len(parts) > 1 else parts[0]
                p = p_ref[head, lower : lower + rows, :keys]
                mixed = jnp.dot(p, v, preferred_element_type=jnp.float32)
                mixed = mixed * t_ref[head, lower : lower + rows, :]
                at = residue + block * rows * stride
                o_all[i, pl.ds(at, rows, stride=stride), :] = mixed

    def copy_of(at):
        lanes = pl.ds(pl.multiple_of((at + first_head) * HS, HS), HS)
        return pltpu.make_async_copy(o_out.at[at], o_ref.at[:, lanes], sems.at[at])

    for i in range(together):
        o_out[step + i] = o_all[i].astype(jnp.bfloat16)
        copy_of(step + i).start()

    @pl.when(pl.program_id(0) == pl.num_programs(0) - 1)
    def _():
        for at in range(o_out.shape[0]):
            copy_of(at).wait()


def body(queries, key_heads, value_heads, dilation, window):
    length, width = queries.shape
    heads_here = width // HS
    assert REACH * length >= 2 ** (LEVELS - 1) * WIN
    count = lax.axis_size("seq")
    bounds = (0, int(SPLIT * heads_here), heads_here)
    whole = pl.BlockSpec(memory_space=pltpu.VMEM)

    def in_hbm(value):
        return pltpu.with_memory_space_constraint(value, pltpu.HBM)

    def send(name, value, both=False):
        return lax.ppermute(value, "seq", routes(count, both)[name.split("_")[0]])

    def call(kernel, steps, scalars, operands, specs, out_specs, out_shape, scratch, **more):
        return pl.pallas_call(
            kernel,
            grid_spec=pltpu.PrefetchScalarGridSpec(
                num_scalar_prefetch=len(scalars),
                grid=(steps,),
                in_specs=specs,
                out_specs=out_specs,
                scratch_shapes=scratch,
            ),
            out_shape=out_shape,
            compiler_params=pltpu.CompilerParams(
                dimension_semantics=("arbitrary",), vmem_limit_bytes=VMEM_LIMIT
            ),
            **more,
        )(*[pltpu.with_memory_space_constraint(scalar, pltpu.SMEM) for scalar in scalars], *operands)

    def by_class(arrays, splits):
        shapes = [
            pltpu.VMEM((length, (high - low) * HS), jnp.bfloat16)
            for parts in splits
            for low, high in parts
        ]
        return call(
            partial(class_kernel, length, splits),
            length // PACK,
            (dilation,),
            [in_hbm(array) for array in arrays],
            [pl.BlockSpec((PACK, width), lambda i, *_: (i, 0))] * len(arrays),
            [whole] * len(shapes),
            shapes,
            [pltpu.VMEM((heads_here, PACK, HS), jnp.float32)],
        )

    keys_most = max(tiling(level, length)[2] for level in range(LEVELS))
    blocks_most = max(length // tiling(l, length)[0] // tiling(l, length)[1] for l in range(LEVELS))
    rows_most = max(tiling(l, length)[1] for l in range(LEVELS))

    two_k = send("two_k", key_heads)
    near_k = send("near_k", key_heads)
    far_k = send("far_k", key_heads)
    relay_k = send("relay_k", near_k)
    keys = (near_k, far_k, relay_k, send("rswap_k", relay_k), two_k, send("swap_k", two_k))

    everything = (0, heads_here)
    own_v, *own_parts = by_class([value_heads], ((everything, bounds[:2], bounds[1:]),))
    far_v = send("far_v", own_v)
    values = []
    for i, part in enumerate(own_parts):
        both = i == 1
        two_v = send(f"two_v{i}", part, both)
        near_v = send(f"near_v{i}", part, both)
        relay_v = send(f"relay_v{i}", near_v, both)
        values.append(
            (
                near_v,
                far_v,
                relay_v,
                send(f"rswap_v{i}", relay_v, both),
                two_v,
                send(f"swap_v{i}", two_v, both),
            )
        )

    class_q, own_k = by_class([queries, key_heads], ((everything,), (everything,)))
    weights, totals = call(
        partial(score_kernel, length, count),
        1,
        (dilation, window),
        (class_q, own_k, *keys),
        [whole] * 8,
        [whole, whole],
        [
            pltpu.VMEM((heads_here, length, keys_most), jnp.bfloat16),
            pltpu.VMEM((heads_here, length, HS), jnp.float32),
        ],
        [
            pltpu.VMEM((heads_here, REACH * length, HS), jnp.float32),
            pltpu.VMEM((blocks_most, rows_most, keys_most), jnp.float32),
        ],
    )
    out = ()
    for i in range(2):
        specs, more = [whole] * 9, {}
        if out:
            specs = specs + [pl.BlockSpec(memory_space=pl.ANY)]
            more = dict(input_output_aliases={10: 0})
        out = (
            call(
                partial(mix_kernel, length, count, bounds[i], i == 1),
                1,
                (dilation,),
                (weights, totals, own_v, *values[i], *out),
                specs,
                pl.BlockSpec(memory_space=pl.ANY),
                jax.ShapeDtypeStruct((length, width), jnp.bfloat16),
                [
                    pltpu.VMEM((bounds[i + 1] - bounds[i], REACH * length, HS), jnp.bfloat16),
                    pltpu.VMEM((bounds[i + 1] - bounds[i], length, HS), jnp.float32),
                    pltpu.VMEM((bounds[i + 1] - bounds[i], length, HS), jnp.bfloat16),
                    pltpu.SemaphoreType.DMA((bounds[i + 1] - bounds[i],)),
                ],
                **more,
            ),
        )
    return out[0]


def solution(mesh):
    return jax.shard_map(
        body,
        mesh=mesh,
        in_specs=(P("seq", "head"), P("seq", "head"), P("seq", "head"), P(), P()),
        out_specs=P("seq", "head"),
        check_vma=False,
    )
```
